32 devices in a mesh: ma: 16 (over z, x, core), ba: 2 (over y).
Axes of the slice: x: 2, y: 2, z: 4, core: 2. Of those that a mesh axis runs over, the one named last changes fastest.
Arguments:
- fields: bfloat16 [4, 256, 256, 192], P('ba', 'ma'), may hold values from -6 to 6
- weight_real: bfloat16 [112, 64, 192, 192], P('ba', 'ma'), may hold values from -0.4375 to 0.4375
- weight_imag: bfloat16 [112, 64, 192, 192], P('ba', 'ma'), may hold values from -0.4375 to 0.4375
- skip_weight: bfloat16 [192, 192], replicated, may hold values from -0.4375 to 0.4375
- out_bias: float32 [192], replicated, may hold values from -3 to 3
Outputs:
- layer_out: bfloat16 [4, 256, 256, 192], P('ba', 'ma')
The draws below stay inside these ranges and needn't reach their ends.
All inputs are finite; a program needn't handle non-finite values.
Results may differ from the reference program's by a relative error of at most 0.0095.
Values may be sent and summed in bfloat16 or wider, within the bound.
A program may use at most 128 MiB of HBM per device.

```python
import math
import jax
import jax.numpy as jnp
from jax import lax

C = 192
H = 256
W = 256
KX = 112
KY = 64
B = 4


def shard_levels(own_key, dims, cuts, low, largest):
    def one(dim, parts):
        heights = jax.random.uniform(jax.random.fold_in(jax.random.fold_in(own_key, 6), dim), (parts,), jnp.float32, low / len(cuts), largest / len(cuts))
        return jnp.repeat(jnp.exp(heights), dims[dim] // parts).reshape((-1,) + (1,) * (len(dims) - dim - 1))

    gain = one(*cuts[0])
    for cut in cuts[1:]:
        gain = gain * one(*cut)
    return gain


def centred(rng, shape, width, reach, cuts=(), kind=jnp.bfloat16):
    loudness = shard_levels(rng, shape, cuts, -0.22, 0.18) if cuts else 1.0
    values = jax.random.normal(rng, shape, jnp.float32) * width * loudness
    return jnp.minimum(jnp.maximum(values, -reach), reach).astype(kind)


def setup_inputs(seed: int = 0) -> dict:
    seeds = jax.random.split(jax.random.key(seed), 6)
    fields = centred(seeds[0], (B, H, W, C), 1.0, 6.0, ((0, 2), (1, 16)))
    weight_real = centred(seeds[1], (KX, KY, C, C), C ** -0.5, 0.4375, ((0, 2), (1, 16)))
    weight_imag = centred(seeds[2], (KX, KY, C, C), C ** -0.5, 0.4375, ((0, 2), (1, 16)))
    skip_weight = centred(seeds[3], (C, C), C ** -0.5, 0.4375)
    out_bias = centred(seeds[4], (C,), 0.5, 3.0, (), jnp.float32)
    return {"fields": fields, "weight_real": weight_real, "weight_imag": weight_imag, "skip_weight": skip_weight, "out_bias": out_bias}


def mode_index(number, extent):
    positions = jnp.arange(number, dtype=jnp.int32)
    return jnp.where(positions < number // 2, positions, positions + (extent - number)).astype(jnp.int32)

def phases(left, right, extent):
    product = left[:, None] * right[None, :] % extent
    angles = 2.0 * math.pi / extent * product.astype(jnp.float32)
    return (jnp.cos(angles), jnp.sin(angles))

def column_tables():
    freqs = jnp.arange(KY, dtype=jnp.int32)
    columns = jnp.arange(W, dtype=jnp.int32)
    cos_kw, sin_kw = phases(freqs, columns, W)
    factor = 1.0 / math.sqrt(H * W)
    col_cos = (cos_kw * factor).T
    col_sin = (-sin_kw * factor).T
    doubled = jnp.where(freqs == 0, 1.0, 2.0).astype(jnp.float32) * factor
    back_cos = cos_kw * doubled[:, None]
    back_sin = -sin_kw * doubled[:, None]
    return (col_cos, col_sin, back_cos, back_sin)

def row_tables():
    freqs = mode_index(KX, H)
    rows = jnp.arange(H, dtype=jnp.int32)
    return phases(freqs, rows, H)

def reference(fields, weight_real, weight_imag, skip_weight, out_bias):
    highest = lax.Precision.HIGHEST
    col_cos, col_sin, back_cos, back_sin = column_tables()
    row_cos, row_sin = row_tables()

    def forward_one(field):
        data = field.astype(jnp.float32)
        col_real = jnp.einsum('hwc,wk->hkc', data, col_cos, precision=highest)
        col_imag = jnp.einsum('hwc,wk->hkc', data, col_sin, precision=highest)
        spec_real = jnp.einsum('ih,hkc->ikc', row_cos, col_real, precision=highest) + jnp.einsum('ih,hkc->ikc', row_sin, col_imag, precision=highest)
        spec_imag = jnp.einsum('ih,hkc->ikc', row_cos, col_imag, precision=highest) - jnp.einsum('ih,hkc->ikc', row_sin, col_real, precision=highest)
        return (spec_real.astype(jnp.bfloat16), spec_imag.astype(jnp.bfloat16))
    spec_real, spec_imag = lax.map(forward_one, fields)

    def mix_one(pieces):
        part_real, part_imag, mode_real, mode_imag = pieces
        part_real = part_real.astype(jnp.float32)
        part_imag = part_imag.astype(jnp.float32)
        mode_real = mode_real.astype(jnp.float32)
        mode_imag = mode_imag.astype(jnp.float32)
        out_real = jnp.einsum('bkc,kco->bko', part_real, mode_real, precision=highest) - jnp.einsum('bkc,kco->bko', part_imag, mode_imag, precision=highest)
        out_imag = jnp.einsum('bkc,kco->bko', part_real, mode_imag, precision=highest) + jnp.einsum('bkc,kco->bko', part_imag, mode_real, precision=highest)
        return (out_real, out_imag)
    mix_real, mix_imag = lax.map(mix_one, (spec_real.transpose(1, 0, 2, 3), spec_imag.transpose(1, 0, 2, 3), weight_real, weight_imag))
    mix_real = mix_real.transpose(1, 0, 2, 3)
    mix_imag = mix_imag.transpose(1, 0, 2, 3)

    def inverse_one(pieces):
        field, part_real, part_imag = pieces
        row_real = jnp.einsum('ih,ikc->hkc', row_cos, part_real, precision=highest) - jnp.einsum('ih,ikc->hkc', row_sin, part_imag, precision=highest)
        row_imag = jnp.einsum('ih,ikc->hkc', row_sin, part_real, precision=highest) + jnp.einsum('ih,ikc->hkc', row_cos, part_imag, precision=highest)
        spectral = jnp.einsum('hkc,kw->hwc', row_real, back_cos, precision=highest) + jnp.einsum('hkc,kw->hwc', row_imag, back_sin, precision=highest)
        skip = jnp.dot(field.reshape(-1, C), skip_weight, preferred_element_type=jnp.float32).reshape(spectral.shape)
        return jax.nn.gelu(spectral + skip + out_bias).astype(jnp.bfloat16)
    return lax.map(inverse_one, (fields, mix_real, mix_imag))
```

```python
import functools
import math

import jax
import jax.numpy as jnp
import numpy as np
from jax import lax
from jax.experimental import pallas as pl
from jax.experimental.pallas import tpu as pltpu
from jax.sharding import PartitionSpec as P

MESH = pl.DeviceIdType.MESH
BF = jnp.bfloat16
F32 = jnp.float32
LANES = 128
VMEM_LIMIT = 67043328


def angles(left, right, extent):
    turn = 2.0 * np.pi / extent * ((left[:, None] * right[None, :]) % extent)
    return np.cos(turn), np.sin(turn)


def packed_tables(H, W, KX, KY, n, nb):
    rows, cols, modes = H // n, KY // n, KX // nb
    s = 1.0 / math.sqrt(H * W)
    ky = np.arange(KY)
    cos_w, sin_w = angles(ky, np.arange(W), W)
    first = np.stack([cos_w * s, -sin_w * s], 1)
    first = first.reshape(n, cols, 2, W).transpose(1, 0, 2, 3).reshape(2 * KY, W)
    g = np.where(ky == 0, 1.0, 2.0)[:, None] * s
    last = np.stack([cos_w * g, -sin_w * g], 1)
    last = last.reshape(n, cols, 2, W).transpose(1, 0, 2, 3).reshape(2 * KY, W).T
    i = np.arange(KX)
    kx = np.where(i < KX // 2, i, i + H - KX)
    cos_h, sin_h = angles(kx, np.arange(H), H)
    down = np.stack([np.stack([cos_h, sin_h], 1), np.stack([-sin_h, cos_h], 1)], 0)
    down = down.reshape(2, nb, modes, 2, n, rows).transpose(1, 0, 2, 4, 3, 5)
    down = down.reshape(2 * KX, 2 * H)
    up = np.stack([np.stack([cos_h, -sin_h], 0), np.stack([sin_h, cos_h], 0)], 0)
    up = up.reshape(2, 2, nb, modes, n, rows).transpose(4, 0, 5, 2, 1, 3).reshape(2 * H, 2 * KX)
    return [jnp.asarray(a.astype(np.float32)).astype(BF) for a in (first, down, up, last)]


def dot(a, b):
    return jnp.dot(a, b, preferred_element_type=F32)


def spectral_kernel(
    n, nb, x_ref, wr_ref, wi_ref, first_ref, down_ref, up_ref, out_ref,
    colf, csend, crecv, ysend, yrecv, m1, m2, mo, zsend, zrecv, rsend, wbuf,
    csem_s, csem_r, ysem_s, ysem_r, zsem_s, zsem_r, rsem_s, rsem_r, wsem,
):
    bl, rows, W, C = x_ref.shape
    cols, _, rows2, L = csend.shape
    modes = wbuf.shape[2]
    K2 = first_ref.shape[0]
    tiles = L // LANES
    slots = wbuf.shape[0]
    group = 2 * nb * bl
    tail = C - LANES
    me = lax.axis_index("ma")
    mine = lax.axis_index("ba")

    def weights(q):
        s = q % slots
        return [
            pltpu.make_async_copy(ref.at[:, q], wbuf.at[s, p], wsem.at[s, p])
            for p, ref in enumerate((wr_ref, wi_ref))
        ]

    for q in range(min(slots, cols)):
        for copy in weights(q):
            copy.start()

    barrier = pltpu.get_barrier_semaphore()
    for j in range(1, n):
        pl.semaphore_signal(
            barrier, inc=1, device_id={"ma": lax.rem(me + j, n)}, device_id_type=MESH
        )
    for j in range(1, nb):
        pl.semaphore_signal(
            barrier, inc=1, device_id={"ba": lax.rem(mine + j, nb)}, device_id_type=MESH
        )

    def over_ma(src, dst, s, r, q, j):
        to = lax.rem(me + j, n)
        return pltpu.make_async_remote_copy(
            src_ref=src.at[q, to], dst_ref=dst.at[q, me], send_sem=s.at[q, j],
            recv_sem=r.at[q, j], device_id={"ma": to}, device_id_type=MESH,
        )

    def over_ba(src, dst, s, r, q, j):
        to = lax.rem(mine + j, nb)
        return pltpu.make_async_remote_copy(
            src_ref=src.at[q, to], dst_ref=dst.at[q, mine], send_sem=s.at[q, j],
            recv_sem=r.at[q, j], device_id={"ba": to}, device_id_type=MESH,
        )

    order = sorted(range(1, n), key=lambda j: -min(j, n - j))

    @pl.loop(0, rows)
    def _(h):
        parts = [dot(first_ref[...], x_ref[b, h]) for b in range(bl)]
        both = jnp.concatenate(parts, axis=1)
        for l in range(tiles):
            colf[l, pl.ds(pl.multiple_of(h * K2, K2), K2), :] = both[:, l * LANES:(l + 1) * LANES]

    sent = []
    for q in range(cols):
        @pl.loop(0, n)
        def _(d, q=q):
            for part in range(2):
                for l in range(tiles):
                    k = q * 2 * n + 2 * d + part
                    v = colf[l, pl.ds(k, rows, stride=K2), :]
                    csend[q, d, part * rows:(part + 1) * rows, l * LANES:(l + 1) * LANES] = v.astype(BF)

        crecv[q, me] = csend[q, me]
        if q == 0:
            pl.semaphore_wait(barrier, n - 1 + nb - 1)
        for j in order:
            c = over_ma(csend, crecv, csem_s, csem_r, q, j)
            c.start()
            sent.append(c)

    ysent, zsent = {}, {}

    def rows_down(q):
        for j in order:
            over_ma(csend, crecv, csem_s, csem_r, q, j).wait_recv()
        col = crecv[q].reshape(n * rows2, L)
        spec = dot(down_ref[...], col).astype(BF)
        for y in range(nb):
            ysend[q, y] = spec[y * 2 * modes:(y + 1) * 2 * modes]
        for j in range(1, nb):
            c = over_ba(ysend, yrecv, ysem_s, ysem_r, q, j)
            c.start()
            sent.append(c)
        yrecv[q, mine] = ysend[q, mine]

    def mix(q):
        for j in range(1, nb):
            over_ba(ysend, yrecv, ysem_s, ysem_r, q, j).wait_recv()
        for y in range(nb):
            whole = yrecv[q, y].astype(F32)
            for part in range(2):
                for b in range(bl):
                    v = whole[part * modes:(part + 1) * modes, b * C:(b + 1) * C]
                    head = v[:, :LANES]
                    rest = jnp.concatenate([v[:, LANES:], jnp.zeros((modes, LANES - tail), F32)], axis=1)
                    r1 = ((part * nb + y) * bl + b) * modes
                    r2 = (((1 - part) * nb + y) * bl + b) * modes
                    m1[0, r1:r1 + modes, :] = head
                    m1[1, r1:r1 + modes, :] = rest
                    m2[0, r2:r2 + modes, :] = head if part == 0 else -head
                    m2[1, r2:r2 + modes, :] = rest if part == 0 else -rest
        for copy in weights(q):
            copy.wait()
        s = q % slots

        def one(i, carry):
            at = pl.ds(i, group, stride=modes)
            a1 = jnp.concatenate([m1[0, at, :], m1[1, at, :][:, :tail]], axis=1).astype(BF)
            a2 = jnp.concatenate([m2[0, at, :], m2[1, at, :][:, :tail]], axis=1).astype(BF)
            o = dot(a1, wbuf[s, 0, i]) + dot(a2, wbuf[s, 1, i])
            mo[0, at, :] = o[:, :LANES]
            mo[1, at, :] = jnp.concatenate([o[:, LANES:], jnp.zeros((group, LANES - tail), F32)], axis=1)
            return carry

        lax.fori_loop(0, modes, one, 0, unroll=UNROLL)
        if q + slots < cols:
            for copy in weights(q + slots):
                copy.start()
        for y in range(nb):
            parts = []
            for part in range(2):
                pieces = []
                for b in range(bl):
                    r = ((part * nb + y) * bl + b) * modes
                    pieces += [mo[0, r:r + modes, :], mo[1, r:r + modes, :][:, :tail]]
                parts.append(jnp.concatenate(pieces, axis=1))
            zsend[q, y] = jnp.concatenate(parts, axis=0).astype(BF)
        for j in range(1, nb):
            c = over_ba(zsend, zrecv, zsem_s, zsem_r, q, j)
            c.start()
            sent.append(c)
        zrecv[q, mine] = zsend[q, mine]

    def rows_up(q):
        for j in range(1, nb):
            over_ba(zsend, zrecv, zsem_s, zsem_r, q, j).wait_recv()
        row = dot(up_ref[...], zrecv[q].reshape(nb * 2 * modes, L))
        rsend[q] = row.astype(BF).reshape(n, rows2, L)
        for j in order:
            c = over_ma(rsend, out_ref, rsem_s, rsem_r, q, j)
            c.start()
            sent.append(c)
        out_ref[q, me] = rsend[q, me]

    for t in range(cols + 2):
        if t < cols:
            rows_down(t)
        if 0 <= t - 2 < cols:
            rows_up(t - 2)
        if 0 <= t - 1 < cols:
            mix(t - 1)
    for q in range(cols):
        for j in order:
            over_ma(rsend, out_ref, rsem_s, rsem_r, q, j).wait_recv()
    for c in sent:
        c.wait_send()


UNROLL = 4


def final_kernel(rr_ref, x_ref, last_ref, skip_ref, bias_ref, out_ref, rf):
    bl, step, W, C = x_ref.shape
    cols, n, rows2, L = rr_ref.shape
    rows = rows2 // 2
    K2 = cols * n * 2
    tiles = L // LANES
    g = pl.program_id(0)

    @pl.when(g == 0)
    def _():
        for q in range(cols):
            @pl.loop(0, n)
            def _(d, q=q):
                v = rr_ref[q, d].astype(F32)
                at = pl.ds(pl.multiple_of((q * n + d) * rows2, rows2), rows2)
                for l in range(tiles):
                    rf[l, at, :] = v[:, l * LANES:(l + 1) * LANES]

    for u in range(step):
        h = g * step + u
        r = jnp.concatenate([rf[l, pl.ds(h, K2, stride=rows), :] for l in range(tiles)], axis=1).astype(BF)
        for b in range(bl):
            v = dot(last_ref[...], r[:, b * C:(b + 1) * C]) + dot(x_ref[b, u], skip_ref[...]) + bias_ref[...]
            inner = math.sqrt(2.0 / math.pi) * (v + 0.044715 * (v * v * v))
            out_ref[b, u] = (0.5 * v * (1.0 + jnp.tanh(inner))).astype(BF)


def kernels(n, nb, H, KX, KY, fields, weight_real, weight_imag, skip_weight, out_bias):
    bl, rows, W, C = fields.shape
    modes, cols = weight_real.shape[:2]
    L, K2 = bl * C, 2 * KY
    first, down, up, last = packed_tables(H, W, KX, KY, n, nb)
    vmem = pl.BlockSpec(memory_space=pltpu.VMEM)
    hbm = pl.BlockSpec(memory_space=pl.ANY)
    tiles = L // LANES
    group = 2 * nb * bl
    ma_block = pltpu.VMEM((cols, n, 2 * rows, L), BF)
    ba_block = pltpu.VMEM((cols, nb, 2 * modes, L), BF)
    mix_block = pltpu.VMEM((2, group * modes, LANES), F32)
    dma = pltpu.SemaphoreType.DMA
    rr = pl.pallas_call(
        functools.partial(spectral_kernel, n, nb),
        out_shape=jax.ShapeDtypeStruct((cols, n, 2 * rows, L), BF),
        in_specs=[vmem, hbm, hbm, vmem, vmem, vmem],
        out_specs=vmem,
        scratch_shapes=[
            pltpu.VMEM((tiles, rows * K2, LANES), F32), ma_block, ma_block, ba_block, ba_block,
            mix_block, mix_block, mix_block, ba_block, ba_block, ma_block,
            pltpu.VMEM((min(2, cols), 2, modes, C, C), BF),
            dma((cols, n)), dma((cols, n)), dma((cols, nb)), dma((cols, nb)), dma((cols, nb)),
            dma((cols, nb)), dma((cols, n)), dma((cols, n)), dma((min(2, cols), 2)),
        ],
        compiler_params=pltpu.CompilerParams(
            collective_id=0, has_side_effects=True, vmem_limit_bytes=VMEM_LIMIT
        ),
        name="spectral",
    )(fields, weight_real, weight_imag, first, down, up)
    step = 2 if rows % 2 == 0 else 1
    slab = pl.BlockSpec((bl, step, W, C), lambda g: (0, g, 0, 0))
    return pl.pallas_call(
        final_kernel,
        grid=(rows // step,),
        out_shape=jax.ShapeDtypeStruct(fields.shape, BF),
        in_specs=[vmem, slab, vmem, vmem, vmem],
        out_specs=slab,
        scratch_shapes=[pltpu.VMEM((tiles, K2 * rows, LANES), F32)],
        compiler_params=pltpu.CompilerParams(vmem_limit_bytes=40 * 2**20),
        name="finish",
    )(rr, fields, last, skip_weight, out_bias.reshape(1, C))


def fits(n, nb, fields, weights):
    bl, rows, W, C = fields.shape
    modes, cols = weights.shape[:2]
    whole = 2 * modes * cols * C * 256 * 2
    return (
        rows % 16 == 0 and modes % 8 == 0 and (bl * C) % LANES == 0 and LANES < C < 2 * LANES
        and 2 * nb * bl == 8 and W % LANES == 0 and whole * min(2, cols) // cols < 36 * 2**20
        and cols * n * 2 % LANES == 0
    )


def any_size(n, nb, H, KX, KY, fields, weight_real, weight_imag, skip_weight, out_bias):
    bl, rows, W, C = fields.shape
    modes, cols = weight_real.shape[:2]
    first, down, up, last = packed_tables(H, W, KX, KY, n, nb)
    col = jnp.einsum("qdpw,brwc->dqprbc", first.reshape(cols, n, 2, W), fields, preferred_element_type=F32)
    col = lax.all_to_all(col.astype(BF), "ma", split_axis=0, concat_axis=0, tiled=True)
    spec = jnp.einsum("ypidrh,dqrhbc->ypqbic", down.reshape(nb, 2, modes, n, 2, rows), col, preferred_element_type=F32)
    spec = lax.all_to_all(spec.astype(BF), "ba", split_axis=0, concat_axis=0, tiled=True)
    re, im = spec[:, 0], spec[:, 1]
    mul = functools.partial(jnp.einsum, "yqbic,iqco->yqbio", preferred_element_type=F32)
    mixed = jnp.stack([
        mul(re, weight_real) - mul(im, weight_imag), mul(re, weight_imag) + mul(im, weight_real)
    ], 1)
    mixed = lax.all_to_all(mixed.astype(BF), "ba", split_axis=0, concat_axis=0, tiled=True)
    row = jnp.einsum("drhypi,ypqbic->dqrhbc", up.reshape(n, 2, rows, nb, 2, modes), mixed, preferred_element_type=F32)
    row = lax.all_to_all(row.astype(BF), "ma", split_axis=0, concat_axis=0, tiled=True)
    spectral = jnp.einsum("wqdr,dqrhbc->bhwc", last.reshape(W, cols, n, 2), row, preferred_element_type=F32)
    skip = jnp.dot(fields.reshape(-1, C), skip_weight, preferred_element_type=F32).reshape(spectral.shape)
    return jax.nn.gelu(spectral + skip + out_bias).astype(BF)


def solution(mesh):
    n, nb = mesh.shape["ma"], mesh.shape["ba"]

    def local(fields, weight_real, weight_imag, skip_weight, out_bias):
        sizes = (fields.shape[1] * n, weight_real.shape[0] * nb, weight_real.shape[1] * n)
        run = kernels if fits(n, nb, fields, weight_real) else any_size
        return run(n, nb, *sizes, fields, weight_real, weight_imag, skip_weight, out_bias)

    split = P("ba", "ma", None, None)
    return jax.shard_map(
        local, mesh=mesh, in_specs=(split, split, split, P(), P()), out_specs=split, check_vma=False
    )
```

```python
import functools
import math

import jax
import jax.numpy as jnp
import numpy as np
from jax import lax
from jax.experimental import pallas as pl
from jax.experimental.pallas import tpu as pltpu
from jax.sharding import PartitionSpec as P

MESH = pl.DeviceIdType.MESH
BF = jnp.bfloat16
F32 = jnp.float32
LANES = 128
VMEM_LIMIT = 67043328


def angles(left, right, extent):
    turn = 2.0 * np.pi / extent * ((left[:, None] * right[None, :]) % extent)
    return np.cos(turn), np.sin(turn)


def packed_tables(H, W, KX, KY, n, nb):
    rows, cols, modes = H // n, KY // n, KX // nb
    s = 1.0 / math.sqrt(H * W)
    ky = np.arange(KY)
    cos_w, sin_w = angles(ky, np.arange(W), W)
    first = np.stack([cos_w * s, -sin_w * s], 1)
    first = first.reshape(n, cols, 2, W).transpose(1, 0, 2, 3).reshape(2 * KY, W)
    g = np.where(ky == 0, 1.0, 2.0)[:, None] * s
    last = np.stack([cos_w * g, -sin_w * g], 1)
    last = last.reshape(n, cols, 2, W).transpose(1, 0, 2, 3).reshape(2 * KY, W)
    i = np.arange(KX)
    kx = np.where(i < KX // 2, i, i + H - KX)
    cos_h, sin_h = angles(kx, np.arange(H), H)
    down = np.stack([np.stack([cos_h, sin_h], 1), np.stack([-sin_h, cos_h], 1)], 0)
    down = down.reshape(2, nb, modes, 2, n, rows).transpose(1, 0, 2, 4, 3, 5)
    down = down.reshape(2 * KX, 2 * H)
    up = np.stack([np.stack([cos_h, -sin_h], 0), np.stack([sin_h, cos_h], 0)], 0)
    up = up.reshape(2, 2, nb, modes, n, rows).transpose(4, 0, 5, 2, 1, 3).reshape(2 * H, 2 * KX)
    return [jnp.asarray(a.astype(np.float32)).astype(BF) for a in (first, down, up, last)]


def dot(a, b, over=(1, 0)):
    return lax.dot_general(a, b, (((over[0],), (over[1],)), ((), ())), preferred_element_type=F32)


def spectral_kernel(
    n, nb, x_ref, wr_ref, wi_ref, first_ref, down_ref, up_ref, out_ref,
    colf, csend, crecv, ysend, yrecv, m1, m2, mo, zsend, zrecv, rsend, wbuf,
    csem_s, csem_r, ysem_s, ysem_r, zsem_s, zsem_r, rsem_s, rsem_r, wsem,
):
    bl, rows, C, W = x_ref.shape
    cols, _, rows2, L = csend.shape
    modes = wbuf.shape[2]
    K2 = first_ref.shape[0]
    tiles = L // LANES
    slots = wbuf.shape[0]
    group = 2 * nb * bl
    tail = C - LANES
    me = lax.axis_index("ma")
    mine = lax.axis_index("ba")

    def weights(q):
        s = q % slots
        return [
            pltpu.make_async_copy(ref.at[:, q], wbuf.at[s, p], wsem.at[s, p])
            for p, ref in enumerate((wr_ref, wi_ref))
        ]

    for q in range(min(slots, cols)):
        for copy in weights(q):
            copy.start()

    barrier = pltpu.get_barrier_semaphore()
    for j in range(1, n):
        pl.semaphore_signal(
            barrier, inc=1, device_id={"ma": lax.rem(me + j, n)}, device_id_type=MESH
        )
    for j in range(1, nb):
        pl.semaphore_signal(
            barrier, inc=1, device_id={"ba": lax.rem(mine + j, nb)}, device_id_type=MESH
        )

    def over_ma(src, dst, s, r, q, j):
        to = lax.rem(me + j, n)
        return pltpu.make_async_remote_copy(
            src_ref=src.at[q, to], dst_ref=dst.at[q, me], send_sem=s.at[q, j],
            recv_sem=r.at[q, j], device_id={"ma": to}, device_id_type=MESH,
        )

    def over_ba(src, dst, s, r, q, j):
        to = lax.rem(mine + j, nb)
        return pltpu.make_async_remote_copy(
            src_ref=src.at[q, to], dst_ref=dst.at[q, mine], send_sem=s.at[q, j],
            recv_sem=r.at[q, j], device_id={"ba": to}, device_id_type=MESH,
        )

    order = sorted(range(1, n), key=lambda j: -min(j, n - j))

    @pl.loop(0, rows)
    def _(h):
        both = dot(first_ref[...], x_ref[:, h].reshape(L, W), (1, 1))
        for l in range(tiles):
            colf[l, pl.ds(pl.multiple_of(h * K2, K2), K2), :] = both[:, l * LANES:(l + 1) * LANES]

    sent = []
    for q in range(cols):
        @pl.loop(0, n)
        def _(d, q=q):
            for part in range(2):
                for l in range(tiles):
                    k = q * 2 * n + 2 * d + part
                    v = colf[l, pl.ds(k, rows, stride=K2), :]
                    csend[q, d, part * rows:(part + 1) * rows, l * LANES:(l + 1) * LANES] = v.astype(BF)

        crecv[q, me] = csend[q, me]
        if q == 0:
            pl.semaphore_wait(barrier, n - 1 + nb - 1)
        for j in order:
            c = over_ma(csend, crecv, csem_s, csem_r, q, j)
            c.start()
            sent.append(c)

    ysent, zsent = {}, {}

    def rows_down(q):
        for j in order:
            over_ma(csend, crecv, csem_s, csem_r, q, j).wait_recv()
        col = crecv[q].reshape(n * rows2, L)
        spec = dot(down_ref[...], col).astype(BF)
        for y in range(nb):
            ysend[q, y] = spec[y * 2 * modes:(y + 1) * 2 * modes]
        for j in range(1, nb):
            c = over_ba(ysend, yrecv, ysem_s, ysem_r, q, j)
            c.start()
            sent.append(c)
        yrecv[q, mine] = ysend[q, mine]

    def mix(q):
        for j in range(1, nb):
            over_ba(ysend, yrecv, ysem_s, ysem_r, q, j).wait_recv()
        for y in range(nb):
            whole = yrecv[q, y].astype(F32)
            for part in range(2):
                for b in range(bl):
                    v = whole[part * modes:(part + 1) * modes, b * C:(b + 1) * C]
                    head = v[:, :LANES]
                    rest = jnp.concatenate([v[:, LANES:], jnp.zeros((modes, LANES - tail), F32)], axis=1)
                    r1 = ((part * nb + y) * bl + b) * modes
                    r2 = (((1 - part) * nb + y) * bl + b) * modes
                    m1[0, r1:r1 + modes, :] = head
                    m1[1, r1:r1 + modes, :] = rest
                    m2[0, r2:r2 + modes, :] = head if part == 0 else -head
                    m2[1, r2:r2 + modes, :] = rest if part == 0 else -rest
        for copy in weights(q):
            copy.wait()
        s = q % slots

        def one(i, carry):
            at = pl.ds(i, group, stride=modes)
            a1 = jnp.concatenate([m1[0, at, :], m1[1, at, :][:, :tail]], axis=1).astype(BF)
            a2 = jnp.concatenate([m2[0, at, :], m2[1, at, :][:, :tail]], axis=1).astype(BF)
            o = dot(a1, wbuf[s, 0, i]) + dot(a2, wbuf[s, 1, i])
            mo[0, at, :] = o[:, :LANES]
            mo[1, at, :] = jnp.concatenate([o[:, LANES:], jnp.zeros((group, LANES - tail), F32)], axis=1)
            return carry

        lax.fori_loop(0, modes, one, 0, unroll=UNROLL)
        if q + slots < cols:
            for copy in weights(q + slots):
                copy.start()
        for y in range(nb):
            parts = []
            for part in range(2):
                pieces = []
                for b in range(bl):
                    r = ((part * nb + y) * bl + b) * modes
                    pieces += [mo[0, r:r + modes, :], mo[1, r:r + modes, :][:, :tail]]
                parts.append(jnp.concatenate(pieces, axis=1))
            zsend[q, y] = jnp.concatenate(parts, axis=0).astype(BF)
        for j in range(1, nb):
            c = over_ba(zsend, zrecv, zsem_s, zsem_r, q, j)
            c.start()
            sent.append(c)
        zrecv[q, mine] = zsend[q, mine]

    def rows_up(q):
        for j in range(1, nb):
            over_ba(zsend, zrecv, zsem_s, zsem_r, q, j).wait_recv()
        row = dot(up_ref[...], zrecv[q].reshape(nb * 2 * modes, L))
        rsend[q] = row.astype(BF).reshape(n, rows2, L)
        for j in order:
            c = over_ma(rsend, out_ref, rsem_s, rsem_r, q, j)
            c.start()
            sent.append(c)
        out_ref[q, me] = rsend[q, me]

    for t in range(cols + 2):
        if t < cols:
            rows_down(t)
        if 0 <= t - 2 < cols:
            rows_up(t - 2)
        if 0 <= t - 1 < cols:
            mix(t - 1)
    for q in range(cols):
        for j in order:
            over_ma(rsend, out_ref, rsem_s, rsem_r, q, j).wait_recv()
    for c in sent:
        c.wait_send()


UNROLL = 4


def final_kernel(rr_ref, x_ref, last_ref, skip_ref, bias_ref, out_ref, rf, turned, biases):
    bl, step, C, W = x_ref.shape
    cols, n, rows2, L = rr_ref.shape
    rows = rows2 // 2
    K2 = cols * n * 2
    tiles = L // LANES
    g = pl.program_id(0)

    @pl.when(g == 0)
    def _():
        turned[...] = skip_ref[...].astype(F32).T.astype(BF)
        wide = jnp.broadcast_to(bias_ref[...], (LANES, C)).T
        for l in range(W // LANES):
            biases[:, l * LANES:(l + 1) * LANES] = wide
        for q in range(cols):
            @pl.loop(0, n)
            def _(d, q=q):
                v = rr_ref[q, d].astype(F32)
                at = pl.ds(pl.multiple_of((q * n + d) * rows2, rows2), rows2)
                for l in range(tiles):
                    rf[l, at, :] = v[:, l * LANES:(l + 1) * LANES]

    for u in range(step):
        h = g * step + u
        r = jnp.concatenate([rf[l, pl.ds(h, K2, stride=rows), :] for l in range(tiles)], axis=1).astype(BF)
        spectral = dot(r, last_ref[...], (0, 0))
        for b in range(bl):
            v = spectral[b * C:(b + 1) * C] + dot(turned[...], x_ref[b, u]) + biases[...]
            inner = math.sqrt(2.0 / math.pi) * (v + 0.044715 * (v * v * v))
            out_ref[b, u] = (0.5 * v * (1.0 + jnp.tanh(inner))).astype(BF)


def kernels(n, nb, H, KX, KY, fields, weight_real, weight_imag, skip_weight, out_bias):
    bl, rows, W, C = fields.shape
    modes, cols = weight_real.shape[:2]
    L, K2 = bl * C, 2 * KY
    first, down, up, last = packed_tables(H, W, KX, KY, n, nb)
    fields = fields.transpose(0, 1, 3, 2)
    vmem = pl.BlockSpec(memory_space=pltpu.VMEM)
    hbm = pl.BlockSpec(memory_space=pl.ANY)
    tiles = L // LANES
    group = 2 * nb * bl
    ma_block = pltpu.VMEM((cols, n, 2 * rows, L), BF)
    ba_block = pltpu.VMEM((cols, nb, 2 * modes, L), BF)
    mix_block = pltpu.VMEM((2, group * modes, LANES), F32)
    dma = pltpu.SemaphoreType.DMA
    rr = pl.pallas_call(
        functools.partial(spectral_kernel, n, nb),
        out_shape=jax.ShapeDtypeStruct((cols, n, 2 * rows, L), BF),
        in_specs=[vmem, hbm, hbm, vmem, vmem, vmem],
        out_specs=vmem,
        scratch_shapes=[
            pltpu.VMEM((tiles, rows * K2, LANES), F32), ma_block, ma_block, ba_block, ba_block,
            mix_block, mix_block, mix_block, ba_block, ba_block, ma_block,
            pltpu.VMEM((min(2, cols), 2, modes, C, C), BF),
            dma((cols, n)), dma((cols, n)), dma((cols, nb)), dma((cols, nb)), dma((cols, nb)),
            dma((cols, nb)), dma((cols, n)), dma((cols, n)), dma((min(2, cols), 2)),
        ],
        compiler_params=pltpu.CompilerParams(
            collective_id=0, has_side_effects=True, vmem_limit_bytes=VMEM_LIMIT
        ),
        name="spectral",
    )(fields, weight_real, weight_imag, first, down, up)
    step = 2 if rows % 2 == 0 else 1
    slab = pl.BlockSpec((bl, step, C, W), lambda g: (0, g, 0, 0))
    out = pl.pallas_call(
        final_kernel,
        grid=(rows // step,),
        out_shape=jax.ShapeDtypeStruct(fields.shape, BF),
        in_specs=[vmem, slab, vmem, vmem, vmem],
        out_specs=slab,
        scratch_shapes=[
            pltpu.VMEM((tiles, K2 * rows, LANES), F32), pltpu.VMEM((C, C), BF), pltpu.VMEM((C, W), F32)
        ],
        compiler_params=pltpu.CompilerParams(vmem_limit_bytes=VMEM_LIMIT),
        name="finish",
    )(rr, fields, last, skip_weight, out_bias.reshape(1, C))
    return out.transpose(0, 1, 3, 2)


def fits(n, nb, fields, weights):
    bl, rows, W, C = fields.shape
    modes, cols = weights.shape[:2]
    whole = 2 * modes * cols * C * 256 * 2
    return (
        rows % 16 == 0 and modes % 8 == 0 and (bl * C) % LANES == 0 and LANES < C < 2 * LANES
        and 2 * nb * bl == 8 and W % LANES == 0 and whole * min(2, cols) // cols < 36 * 2**20
        and cols * n * 2 % LANES == 0
    )


def any_size(n, nb, H, KX, KY, fields, weight_real, weight_imag, skip_weight, out_bias):
    bl, rows, W, C = fields.shape
    modes, cols = weight_real.shape[:2]
    first, down, up, last = packed_tables(H, W, KX, KY, n, nb)
    col = jnp.einsum("qdpw,brwc->dqprbc", first.reshape(cols, n, 2, W), fields, preferred_element_type=F32)
    col = lax.all_to_all(col.astype(BF), "ma", split_axis=0, concat_axis=0, tiled=True)
    spec = jnp.einsum("ypidrh,dqrhbc->ypqbic", down.reshape(nb, 2, modes, n, 2, rows), col, preferred_element_type=F32)
    spec = lax.all_to_all(spec.astype(BF), "ba", split_axis=0, concat_axis=0, tiled=True)
    re, im = spec[:, 0], spec[:, 1]
    mul = functools.partial(jnp.einsum, "yqbic,iqco->yqbio", preferred_element_type=F32)
    mixed = jnp.stack([
        mul(re, weight_real) - mul(im, weight_imag), mul(re, weight_imag) + mul(im, weight_real)
    ], 1)
    mixed = lax.all_to_all(mixed.astype(BF), "ba", split_axis=0, concat_axis=0, tiled=True)
    row = jnp.einsum("drhypi,ypqbic->dqrhbc", up.reshape(n, 2, rows, nb, 2, modes), mixed, preferred_element_type=F32)
    row = lax.all_to_all(row.astype(BF), "ma", split_axis=0, concat_axis=0, tiled=True)
    spectral = jnp.einsum("qdrw,dqrhbc->bhwc", last.reshape(cols, n, 2, W), row, preferred_element_type=F32)
    skip = jnp.dot(fields.reshape(-1, C), skip_weight, preferred_element_type=F32).reshape(spectral.shape)
    return jax.nn.gelu(spectral + skip + out_bias).astype(BF)


def solution(mesh):
    n, nb = mesh.shape["ma"], mesh.shape["ba"]

    def local(fields, weight_real, weight_imag, skip_weight, out_bias):
        sizes = (fields.shape[1] * n, weight_real.shape[0] * nb, weight_real.shape[1] * n)
        run = kernels if fits(n, nb, fields, weight_real) else any_size
        return run(n, nb, *sizes, fields, weight_real, weight_imag, skip_weight, out_bias)

    split = P("ba", "ma", None, None)
    return jax.shard_map(
        local, mesh=mesh, in_specs=(split, split, split, P(), P()), out_specs=split, check_vma=False
    )
```

```python
import functools
import math

import jax
import jax.numpy as jnp
import numpy as np
from jax import lax
from jax.experimental import pallas as pl
from jax.experimental.pallas import tpu as pltpu
from jax.sharding import PartitionSpec as P

MESH = pl.DeviceIdType.MESH
BF = jnp.bfloat16
F32 = jnp.float32
LANES = 128
VMEM_LIMIT = 67043328


def angles(left, right, extent):
    turn = 2.0 * np.pi / extent * ((left[:, None] * right[None, :]) % extent)
    return np.cos(turn), np.sin(turn)


def packed_tables(H, W, KX, KY, n, nb):
    rows, cols, modes = H // n, KY // n, KX // nb
    s = 1.0 / math.sqrt(H * W)
    ky = np.arange(KY)
    cos_w, sin_w = angles(ky, np.arange(W), W)
    first = np.stack([cos_w * s, -sin_w * s], 1)
    first = first.reshape(n, cols, 2, W).transpose(1, 0, 2, 3).reshape(2 * KY, W)
    g = np.where(ky == 0, 1.0, 2.0)[:, None] * s
    last = np.stack([cos_w * g, -sin_w * g], 1)
    last = last.reshape(n, cols, 2, W).transpose(1, 2, 0, 3).reshape(2 * KY, W)
    i = np.arange(KX)
    kx = np.where(i < KX // 2, i, i + H - KX)
    cos_h, sin_h = angles(kx, np.arange(H), H)
    down = np.stack([np.stack([cos_h, sin_h], 1), np.stack([-sin_h, cos_h], 1)], 0)
    down = down.reshape(2, nb, modes, 2, n, rows).transpose(1, 0, 2, 4, 3, 5)
    down = down.reshape(2 * KX, 2 * H)
    up = np.stack([np.stack([cos_h, -sin_h], 0), np.stack([sin_h, cos_h], 0)], 0)
    up = up.reshape(2, 2, nb, modes, n, 2, rows // 2).transpose(4, 5, 0, 6, 2, 1, 3)
    up = up.reshape(2 * H, 2 * KX)
    return [jnp.asarray(a.astype(np.float32)).astype(BF) for a in (first, down, up, last)]


def dot(a, b, over=(1, 0)):
    return lax.dot_general(a, b, (((over[0],), (over[1],)), ((), ())), preferred_element_type=F32)


def spectral_kernel(
    n, nb, x_ref, wr_ref, wi_ref, first_ref, down_ref, up_ref, last_ref, skip_ref, bias_ref, out_ref,
    colf, csend, crecv, ysend, yrecv, m1, m2, mo, zsend, zrecv, rsend, rrecv, wbuf,
    xbuf, acc, obuf, rf, turned, biases,
    csem_s, csem_r, ysem_s, ysem_r, zsem_s, zsem_r, rsem_s, rsem_r, wsem, xsem, osem,
):
    bl, rows, C, W = x_ref.shape
    cols, _, rows2, L = csend.shape
    modes = wbuf.shape[2]
    K2 = first_ref.shape[0]
    tiles = L // LANES
    slots = wbuf.shape[0]
    group = 2 * nb * bl
    tail = C - LANES
    me = lax.axis_index("ma")
    mine = lax.axis_index("ba")

    def weights(q):
        s = q % slots
        return [
            pltpu.make_async_copy(ref.at[:, q], wbuf.at[s, p], wsem.at[s, p])
            for p, ref in enumerate((wr_ref, wi_ref))
        ]

    def loads(g):
        at = pl.ds(g * PIECE, PIECE)
        return pltpu.make_async_copy(x_ref.at[:, at], xbuf.at[:, at], xsem.at[g])

    def stores(g):
        at = pl.ds(g * PIECE, PIECE)
        return pltpu.make_async_copy(obuf.at[:, at], out_ref.at[:, at], osem.at[g])

    barrier = pltpu.get_barrier_semaphore()
    for j in range(1, n):
        pl.semaphore_signal(
            barrier, inc=1, device_id={"ma": lax.rem(me + j, n)}, device_id_type=MESH
        )
    for j in range(1, nb):
        pl.semaphore_signal(
            barrier, inc=1, device_id={"ba": lax.rem(mine + j, nb)}, device_id_type=MESH
        )

    def over_ma(src, dst, s, r, q, j):
        to = lax.rem(me + j, n)
        return pltpu.make_async_remote_copy(
            src_ref=src.at[q, to], dst_ref=dst.at[q, me], send_sem=s.at[q, j],
            recv_sem=r.at[q, j], device_id={"ma": to}, device_id_type=MESH,
        )

    def over_ba(src, dst, s, r, q, j):
        to = lax.rem(mine + j, nb)
        return pltpu.make_async_remote_copy(
            src_ref=src.at[q, to], dst_ref=dst.at[q, mine], send_sem=s.at[q, j],
            recv_sem=r.at[q, j], device_id={"ba": to}, device_id_type=MESH,
        )

    for g in range(rows // PIECE):
        loads(g).start()
    for q in range(min(slots, cols)):
        for copy in weights(q):
            copy.start()

    order = sorted(range(1, n), key=lambda j: -min(j, n - j))

    for g in range(rows // PIECE):
        loads(g).wait()

        @pl.loop(g * PIECE, (g + 1) * PIECE)
        def _(h):
            both = dot(first_ref[...], xbuf[:, h].reshape(L, W), (1, 1))
            for l in range(tiles):
                colf[l, pl.ds(pl.multiple_of(h * K2, K2), K2), :] = both[:, l * LANES:(l + 1) * LANES]

    sent = []
    for q in range(cols):
        @pl.loop(0, n)
        def _(d, q=q):
            for part in range(2):
                for l in range(tiles):
                    k = q * 2 * n + 2 * d + part
                    v = colf[l, pl.ds(k, rows, stride=K2), :]
                    csend[q, d, part * rows:(part + 1) * rows, l * LANES:(l + 1) * LANES] = v.astype(BF)

        crecv[q, me] = csend[q, me]
        if q == 0:
            pl.semaphore_wait(barrier, n - 1 + nb - 1)
        for j in order:
            c = over_ma(csend, crecv, csem_s, csem_r, q, j)
            c.start()
            sent.append(c)

    ysent, zsent = {}, {}

    def rows_down(q):
        for j in order:
            over_ma(csend, crecv, csem_s, csem_r, q, j).wait_recv()
        col = crecv[q].reshape(n * rows2, L)
        spec = dot(down_ref[...], col).astype(BF)
        for y in range(nb):
            ysend[q, y] = spec[y * 2 * modes:(y + 1) * 2 * modes]
        for j in range(1, nb):
            c = over_ba(ysend, yrecv, ysem_s, ysem_r, q, j)
            c.start()
            sent.append(c)
        yrecv[q, mine] = ysend[q, mine]

    def mix(q):
        for j in range(1, nb):
            over_ba(ysend, yrecv, ysem_s, ysem_r, q, j).wait_recv()
        for y in range(nb):
            whole = yrecv[q, y].astype(F32)
            for part in range(2):
                for b in range(bl):
                    v = whole[part * modes:(part + 1) * modes, b * C:(b + 1) * C]
                    head = v[:, :LANES]
                    rest = jnp.concatenate([v[:, LANES:], jnp.zeros((modes, LANES - tail), F32)], axis=1)
                    r1 = ((part * nb + y) * bl + b) * modes
                    r2 = (((1 - part) * nb + y) * bl + b) * modes
                    m1[0, r1:r1 + modes, :] = head
                    m1[1, r1:r1 + modes, :] = rest
                    m2[0, r2:r2 + modes, :] = head if part == 0 else -head
                    m2[1, r2:r2 + modes, :] = rest if part == 0 else -rest
        for copy in weights(q):
            copy.wait()
        s = q % slots

        def one(i, carry):
            at = pl.ds(i, group, stride=modes)
            a1 = jnp.concatenate([m1[0, at, :], m1[1, at, :][:, :tail]], axis=1).astype(BF)
            a2 = jnp.concatenate([m2[0, at, :], m2[1, at, :][:, :tail]], axis=1).astype(BF)
            o = dot(a1, wbuf[s, 0, i]) + dot(a2, wbuf[s, 1, i])
            mo[0, at, :] = o[:, :LANES]
            mo[1, at, :] = jnp.concatenate([o[:, LANES:], jnp.zeros((group, LANES - tail), F32)], axis=1)
            return carry

        lax.fori_loop(0, modes, one, 0, unroll=UNROLL)
        if q + slots < cols:
            for copy in weights(q + slots):
                copy.start()
        for y in range(nb):
            parts = []
            for part in range(2):
                pieces = []
                for b in range(bl):
                    r = ((part * nb + y) * bl + b) * modes
                    pieces += [mo[0, r:r + modes, :], mo[1, r:r + modes, :][:, :tail]]
                parts.append(jnp.concatenate(pieces, axis=1))
            zsend[q, y] = jnp.concatenate(parts, axis=0).astype(BF)
        for j in range(1, nb):
            c = over_ba(zsend, zrecv, zsem_s, zsem_r, q, j)
            c.start()
            sent.append(c)
        zrecv[q, mine] = zsend[q, mine]

    def rows_up(q):
        for j in range(1, nb):
            over_ba(zsend, zrecv, zsem_s, zsem_r, q, j).wait_recv()
        row = dot(up_ref[...], zrecv[q].reshape(nb * 2 * modes, L))
        rsend[q] = row.astype(BF).reshape(n, rows2, L)
        for half in halves(q):
            for j in order:
                c = back(q, j, half)
                c.start()
                sent.append(c)
        rrecv[q, me] = rsend[q, me]

    def halves(q):
        return (0, 1) if q == cols - 1 else (None,)

    def back(q, j, half):
        if half is None:
            return over_ma(rsend, rrecv, rsem_s, rsem_r, q, j)
        to = lax.rem(me + j, n)
        at = pl.ds(half * rows, rows)
        return pltpu.make_async_remote_copy(
            src_ref=rsend.at[q, to, at], dst_ref=rrecv.at[q, me, at],
            send_sem=rsem_s.at[q + half, j], recv_sem=rsem_r.at[q + half, j],
            device_id={"ma": to}, device_id_type=MESH,
        )

    def pointwise():
        turned[...] = skip_ref[...].astype(F32).T.astype(BF)
        wide = jnp.broadcast_to(bias_ref[...], (LANES, C)).T
        for l in range(W // LANES):
            biases[:, l * LANES:(l + 1) * LANES] = wide

        @pl.loop(0, rows)
        def _(h):
            for b in range(bl):
                acc[h, b * C:(b + 1) * C, :] = dot(turned[...], xbuf[b, h]) + biases[...]

    def columns_back(q):
        final = q == cols - 1
        for half in halves(q):
            for j in order:
                back(q, j, half).wait_recv()

            @pl.loop(0, n)
            def _(d):
                v = rrecv[q, d].astype(F32) if half is None else rrecv[q, d, half * rows:(half + 1) * rows].astype(F32)
                size = v.shape[0]
                at = pl.ds(pl.multiple_of(d * rows2 + (half or 0) * rows, rows), size)
                for l in range(tiles):
                    rf[l, at, :] = v[:, l * LANES:(l + 1) * LANES]

            table = last_ref[q * 2 * n:(q + 1) * 2 * n]
            for e in (0, 1) if half is None else (half,):
                for g in range(rows // 2 // PIECE):
                    @pl.loop(0, PIECE)
                    def _(i):
                        low = g * PIECE + i
                        h = e * (rows // 2) + low
                        r = jnp.concatenate([
                            jnp.concatenate([
                                rf[l, pl.ds(e * rows + part * (rows // 2) + low, n, stride=rows2), :]
                                for l in range(tiles)
                            ], axis=1) for part in range(2)
                        ], axis=0).astype(BF)
                        spectral = dot(r, table, (0, 0))
                        for b in range(bl):
                            v = acc[h, b * C:(b + 1) * C, :] + spectral[b * C:(b + 1) * C]
                            if not final:
                                acc[h, b * C:(b + 1) * C, :] = v
                                continue
                            inner = math.sqrt(2.0 / math.pi) * (v + 0.044715 * (v * v * v))
                            obuf[b, h] = (0.5 * v * (1.0 + jnp.tanh(inner))).astype(BF)

                    if final:
                        stores(e * (rows // 2 // PIECE) + g).start()

    pointwise()
    for t in range(cols + 1):
        if t < cols:
            rows_down(t)
        if t >= 1:
            rows_up(t - 1)
        if t < cols:
            mix(t)
    for q in range(cols):
        columns_back(q)
    for c in sent:
        c.wait_send()
    for g in range(rows // PIECE):
        stores(g).wait()


PIECE = 4
UNROLL = 4


def kernels(n, nb, H, KX, KY, fields, weight_real, weight_imag, skip_weight, out_bias):
    bl, rows, W, C = fields.shape
    modes, cols = weight_real.shape[:2]
    L, K2 = bl * C, 2 * KY
    first, down, up, last = packed_tables(H, W, KX, KY, n, nb)
    fields = fields.transpose(0, 1, 3, 2)
    vmem = pl.BlockSpec(memory_space=pltpu.VMEM)
    hbm = pl.BlockSpec(memory_space=pl.ANY)
    tiles = L // LANES
    group = 2 * nb * bl
    ma_block = pltpu.VMEM((cols, n, 2 * rows, L), BF)
    ba_block = pltpu.VMEM((cols, nb, 2 * modes, L), BF)
    mix_block = pltpu.VMEM((2, group * modes, LANES), F32)
    dma = pltpu.SemaphoreType.DMA
    out = pl.pallas_call(
        functools.partial(spectral_kernel, n, nb),
        out_shape=jax.ShapeDtypeStruct(fields.shape, BF),
        in_specs=[hbm, hbm, hbm, vmem, vmem, vmem, vmem, vmem, vmem],
        out_specs=hbm,
        scratch_shapes=[
            pltpu.VMEM((tiles, rows * K2, LANES), F32), ma_block, ma_block, ba_block, ba_block,
            mix_block, mix_block, mix_block, ba_block, ba_block, ma_block, ma_block,
            pltpu.VMEM((min(2, cols), 2, modes, C, C), BF),
            pltpu.VMEM((bl, rows, C, W), BF), pltpu.VMEM((rows, L, W), F32), pltpu.VMEM((bl, rows, C, W), BF),
            pltpu.VMEM((tiles, n * 2 * rows, LANES), F32), pltpu.VMEM((C, C), BF), pltpu.VMEM((C, W), F32),
            dma((cols, n)), dma((cols, n)), dma((cols, nb)), dma((cols, nb)), dma((cols, nb)),
            dma((cols, nb)), dma((cols + 1, n)), dma((cols + 1, n)), dma((min(2, cols), 2)),
            dma((rows // PIECE,)), dma((rows // PIECE,)),
        ],
        compiler_params=pltpu.CompilerParams(
            collective_id=0, has_side_effects=True, vmem_limit_bytes=VMEM_LIMIT
        ),
        name="spectral",
    )(fields, weight_real, weight_imag, first, down, up, last, skip_weight, out_bias.reshape(1, C))
    return out.transpose(0, 1, 3, 2)


def fits(n, nb, fields, weights):
    bl, rows, W, C = fields.shape
    modes, cols = weights.shape[:2]
    whole = 2 * modes * cols * C * 256 * 2
    return (
        rows % 16 == 0 and modes % 8 == 0 and (bl * C) % LANES == 0 and LANES < C < 2 * LANES
        and 2 * nb * bl == 8 and W % LANES == 0 and whole * min(2, cols) // cols < 36 * 2**20
        and cols * n * 2 % LANES == 0
    )


def any_size(n, nb, H, KX, KY, fields, weight_real, weight_imag, skip_weight, out_bias):
    bl, rows, W, C = fields.shape
    modes, cols = weight_real.shape[:2]
    first, down, up, last = packed_tables(H, W, KX, KY, n, nb)
    col = jnp.einsum("qdpw,brwc->dqprbc", first.reshape(cols, n, 2, W), fields, preferred_element_type=F32)
    col = lax.all_to_all(col.astype(BF), "ma", split_axis=0, concat_axis=0, tiled=True)
    spec = jnp.einsum("ypidrh,dqrhbc->ypqbic", down.reshape(nb, 2, modes, n, 2, rows), col, preferred_element_type=F32)
    spec = lax.all_to_all(spec.astype(BF), "ba", split_axis=0, concat_axis=0, tiled=True)
    re, im = spec[:, 0], spec[:, 1]
    mul = functools.partial(jnp.einsum, "yqbic,iqco->yqbio", preferred_element_type=F32)
    mixed = jnp.stack([
        mul(re, weight_real) - mul(im, weight_imag), mul(re, weight_imag) + mul(im, weight_real)
    ], 1)
    mixed = lax.all_to_all(mixed.astype(BF), "ba", split_axis=0, concat_axis=0, tiled=True)
    row = jnp.einsum("derhypi,ypqbic->dqrehbc", up.reshape(n, 2, 2, rows // 2, nb, 2, modes), mixed, preferred_element_type=F32)
    row = lax.all_to_all(row.astype(BF), "ma", split_axis=0, concat_axis=0, tiled=True)
    spectral = jnp.einsum("qrdw,dqrehbc->behwc", last.reshape(cols, 2, n, W), row, preferred_element_type=F32)
    spectral = spectral.reshape(fields.shape)
    skip = jnp.dot(fields.reshape(-1, C), skip_weight, preferred_element_type=F32).reshape(spectral.shape)
    return jax.nn.gelu(spectral + skip + out_bias).astype(BF)


def solution(mesh):
    n, nb = mesh.shape["ma"], mesh.shape["ba"]

    def local(fields, weight_real, weight_imag, skip_weight, out_bias):
        sizes = (fields.shape[1] * n, weight_real.shape[0] * nb, weight_real.shape[1] * n)
        run = kernels if fits(n, nb, fields, weight_real) else any_size
        return run(n, nb, *sizes, fields, weight_real, weight_imag, skip_weight, out_bias)

    split = P("ba", "ma", None, None)
    return jax.shard_map(
        local, mesh=mesh, in_specs=(split, split, split, P(), P()), out_specs=split, check_vma=False
    )
```
